32 devices in a mesh: fsdp: 8 (over y, x, core), tensor: 4 (over z).
Axes of the slice: x: 2, y: 2, z: 4, core: 2. Of those that a mesh axis runs over, the one named last changes fastest.
Arguments:
- tokens: bfloat16 [8192, 2048], P(('fsdp', 'tensor')), may hold values from -6 to 6
- segment_ids: int32 [8, 1024], P('fsdp'), may hold values from 0 to 3, never falling along the last dimension, each value on 1 to 800 neighbouring positions
- attention_gain: bfloat16 [2048], P('fsdp'), may hold values from 0.25 to 1.75
- attention_shift: bfloat16 [2048], P('fsdp'), may hold values from -1.75 to 1.75
- heads_weight: bfloat16 [3, 2048, 2048], P(None, 'fsdp', 'tensor'), may hold values from -0.125 to 0.125
- heads_bias: bfloat16 [2, 2048], P(None, ('tensor', 'fsdp')), may hold values from -3 to 3
- output_weight: bfloat16 [2048, 2048], P('tensor', 'fsdp'), may hold values from -0.5 to 0.5
- output_bias: bfloat16 [2048], P('fsdp'), may hold values from -1.75 to 1.75
- feed_gain: bfloat16 [2048], P('fsdp'), may hold values from 0.25 to 1.75
- feed_shift: bfloat16 [2048], P('fsdp'), may hold values from -1.75 to 1.75
- upward_weight: bfloat16 [2048, 8192], P('fsdp', 'tensor'), may hold values from -0.125 to 0.125
- upward_bias: bfloat16 [8192], P(('tensor', 'fsdp')), may hold values from -3 to 3
- down_weight: bfloat16 [8192, 2048], P('tensor', 'fsdp'), may hold values from -0.0625 to 0.0625
- down_bias: bfloat16 [2048], P('fsdp'), may hold values from -1.75 to 1.75
- cotangent: bfloat16 [8192, 2048], P(('fsdp', 'tensor')), may hold values from -12 to 12
Outputs:
- layer_output: bfloat16 [8192, 2048], P(('fsdp', 'tensor'))
- input_grad: bfloat16 [8192, 2048], P(('fsdp', 'tensor'))
- attention_gain_grad: float32 [2048], P('fsdp')
- attention_shift_grad: float32 [2048], P('fsdp')
- heads_weight_grad: float32 [3, 2048, 2048], P(None, 'fsdp', 'tensor')
- heads_bias_grad: float32 [2, 2048], P(None, ('tensor', 'fsdp'))
- output_weight_grad: float32 [2048, 2048], P('tensor', 'fsdp')
- output_bias_grad: float32 [2048], P('fsdp')
- feed_gain_grad: float32 [2048], P('fsdp')
- feed_shift_grad: float32 [2048], P('fsdp')
- upward_weight_grad: float32 [2048, 8192], P('fsdp', 'tensor')
- upward_bias_grad: float32 [8192], P(('tensor', 'fsdp'))
- down_weight_grad: float32 [8192, 2048], P('tensor', 'fsdp')
- down_bias_grad: float32 [2048], P('fsdp')
The draws below stay inside these ranges and needn't reach their ends.
Inputs may be any that keep to these rules, and one draw needn't show every extreme that they name: `segment_ids`: within each sequence the ids never fall; each id covers 1 to 800 consecutive tokens, and some id covers exactly 800.
All inputs are finite; a program needn't handle non-finite values.
Results may differ from the reference program's by a relative error of at most 0.015.
Values may be sent and summed in bfloat16 or wider, within the bound.
A program may use at most 192 MiB of HBM per device.

```python
import math
import jax
import jax.numpy as jnp
import numpy as np
from jax import lax

D = 2048
HEADS = 16
HD = 128
FF = 8192
SEQ_LEN = 1024
DOC_COUNT = 4
DOC_MOST = 800
GROUP_SEQS = 1
SEQS = 8
TOKENS = 8192


def strengthened(array, rng, source, target, blocks, factor):
    owner, partner = [(jnp.arange(array.shape[axis_at]) // (array.shape[axis_at] // blocks)).reshape([-1 if axis == axis_at else 1 for axis in range(array.ndim)]) for axis_at in (source, target)]
    chosen = jax.random.permutation(rng, blocks)[partner]
    strong = (owner == chosen) | (owner == (partner + blocks // 2) % blocks)
    return jnp.where(strong, factor * array, array)


def levels(rng, dims, shards, smallest, top_value):
    factor_of, own = 1.0, jax.random.fold_in(rng, 6)
    for dim, shards_of in shards:
        heights = jnp.exp(jax.random.uniform(jax.random.fold_in(own, dim), (shards_of,), jnp.float32, smallest / len(shards), top_value / len(shards)))
        factor_of = factor_of * jnp.repeat(heights, dims[dim] // shards_of).reshape([-1 if axis == dim else 1 for axis in range(len(dims))])
    return factor_of


def profile(count, total, bound, lean):
    weights = [(1 << 20) // math.isqrt(grade ** lean) + 1 for grade in range(2, count + 1)]
    rest, given = total - bound - (count - 1), [1] * (count - 1)
    while rest > 0:
        movable = [i for i in range(count - 1) if given[i] < bound]
        mass, left = sum([weights[i] for i in movable]), rest
        for i in movable:
            more = min(bound - given[i], max(1, left * weights[i] // mass), rest)
            given[i] = given[i] + more
            rest = rest - more
    return np.array([bound] + given)


def ragged(own_key, amount, total, limit, skew):
    if amount == 2:
        one = jax.random.randint(own_key, (), max(1, total - limit), min(limit, total - 1) + 1)
        return jnp.stack([one, total - one])
    sizes = jnp.asarray(profile(amount, total, limit, skew), jnp.int32)
    twos = (amount - 1) // 2
    donor, receiver = sizes[1:1 + 2 * twos:2], sizes[2:2 + 2 * twos:2]
    margin = jnp.minimum(donor - 1, limit - receiver)
    shifted = jax.random.randint(jax.random.fold_in(own_key, 1), (twos,), 0, 1 << 20) % (margin + 1)
    sizes = sizes.at[1:1 + 2 * twos:2].set(donor - shifted).at[2:2 + 2 * twos:2].set(receiver + shifted)
    return sizes[jax.random.permutation(jax.random.fold_in(own_key, 2), amount)]


def scatter_about(stream_key, extent, scale, bound, cuts=(), dtype=jnp.bfloat16):
    level = levels(stream_key, extent, cuts, -0.22, 0.18) if cuts else 1.0
    array = jax.random.normal(stream_key, extent, jnp.float32) * scale * level
    return jnp.minimum(jnp.maximum(array, -bound), bound).astype(dtype)


def heavy_noise(rng, dims, width, limit, split, heavy, kind=jnp.bfloat16):
    drawn = width * jax.random.normal(rng, dims, jnp.float32)
    if split:
        drawn = drawn * levels(rng, dims, split, -0.22, 0.18)
    return jnp.clip(strengthened(drawn, jax.random.fold_in(rng, 3), *heavy), -limit, limit).astype(kind)


def setup_inputs(seed: int = 0) -> dict:
    key_of = jax.random.split(jax.random.key(seed), 16)
    tokens = scatter_about(key_of[0], (TOKENS, D), 1.0, 6.0, ((0, 32),))
    segment_ids = jax.vmap(lambda own: jnp.searchsorted(jnp.cumsum(ragged(own, DOC_COUNT, SEQ_LEN, DOC_MOST, 1)), jnp.arange(SEQ_LEN), side="right"))(jax.random.split(key_of[1], SEQS)).reshape((SEQS, SEQ_LEN)).astype(jnp.int32)
    attention_gain = jnp.clip(1.0 + 0.15 * jax.random.normal(key_of[2], (D,), jnp.float32), 0.25, 1.75).astype(jnp.bfloat16)
    attention_shift = scatter_about(key_of[3], (D,), 0.3, 1.75, ((0, 8),))
    heads_weight = scatter_about(key_of[4], (3, D, D), D ** -0.5, 0.125, ((1, 8), (2, 4)))
    heads_bias = scatter_about(key_of[5], (2, D), 0.5, 3.0, ((1, 32),))
    output_weight = scatter_about(key_of[6], (D, D), (D // 16) ** -0.5, 0.5, ((0, 4), (1, 8)))
    output_bias = scatter_about(key_of[7], (D,), 0.3, 1.75, ((0, 8),))
    feed_gain = jnp.clip(1.0 + 0.15 * jax.random.normal(key_of[8], (D,), jnp.float32), 0.25, 1.75).astype(jnp.bfloat16)
    feed_shift = scatter_about(key_of[9], (D,), 0.3, 1.75, ((0, 8),))
    upward_weight = scatter_about(key_of[10], (D, FF), D ** -0.5, 0.125, ((0, 8), (1, 4)))
    upward_bias = scatter_about(key_of[11], (FF,), 0.5, 3.0, ((0, 32),))
    down_weight = scatter_about(key_of[12], (FF, D), FF ** -0.5, 0.0625, ((0, 4), (1, 8)))
    down_bias = scatter_about(key_of[13], (D,), 0.3, 1.75, ((0, 8),))
    cotangent = heavy_noise(key_of[14], (TOKENS, D), 1.0, 12.0, ((0, 32),), (0, 1, 32, 2.75))
    return {"tokens": tokens, "segment_ids": segment_ids, "attention_gain": attention_gain, "attention_shift": attention_shift, "heads_weight": heads_weight, "heads_bias": heads_bias, "output_weight": output_weight, "output_bias": output_bias, "feed_gain": feed_gain, "feed_shift": feed_shift, "upward_weight": upward_weight, "upward_bias": upward_bias, "down_weight": down_weight, "down_bias": down_bias, "cotangent": cotangent}


@jax.custom_vjp
def low(v):
    return lax.optimization_barrier(v.astype(jnp.bfloat16)).astype(jnp.float32)

@jax.custom_vjp
def low_back(v):
    return v

def low_keep(v):
    return (low(v), None)

def low_pass(kept, grad):
    return (grad,)

def back_keep(v):
    return (v, None)

def back_low(kept, grad):
    return (low(grad),)
low.defvjp(low_keep, low_pass)
low_back.defvjp(back_keep, back_low)
EPSILON = 1e-05
NEGATIVE = -1e+30

def product(former, latter):
    return jnp.dot(former, latter, precision=lax.Precision.HIGHEST)

def layer_norm(values_in, gain, shift):
    center = values_in - lax.optimization_barrier(jnp.mean(values_in, axis=-1, keepdims=True))
    spread = lax.optimization_barrier(jnp.mean(center * center, axis=-1, keepdims=True))
    return center * lax.rsqrt(spread + EPSILON) * gain + shift

def attend_one(inputs):
    queries, keys_all, values_all, segments = inputs
    scaling = HD ** (-0.5)
    scores = jnp.einsum('qhd,khd->hqk', queries, keys_all, precision=lax.Precision.HIGHEST) * scaling
    scores = low_back(scores)
    places = jnp.arange(SEQ_LEN)
    allowed = (segments[:, None] == segments[None, :]) & (places[None, :] <= places[:, None])
    scores = jnp.where(allowed[None], scores, NEGATIVE)
    weights = jax.nn.softmax(scores, axis=-1)
    return jnp.einsum('hqk,khd->qhd', low(weights), values_all, precision=lax.Precision.HIGHEST)

def forward(inputs, param_set, segments):
    attention_gain, attention_shift, heads_weight, heads_bias, output_weight, output_bias, feed_gain, feed_shift, upward_weight, upward_bias, down_weight, down_bias = param_set
    normed = low(layer_norm(inputs, attention_gain, attention_shift))
    queries = low(low_back(product(normed, heads_weight[0]) + heads_bias[0]))
    keys_all = low(low_back(product(normed, heads_weight[1])))
    values_all = low(low_back(product(normed, heads_weight[2]) + heads_bias[1]))
    seq_count = segments.shape[0]

    def shaped(tensor_in):
        return tensor_in.reshape(seq_count, SEQ_LEN, HEADS, HD)
    context = lax.map(jax.checkpoint(attend_one), (shaped(queries), shaped(keys_all), shaped(values_all), segments))
    context = low(low_back(context.reshape(inputs.shape[0], D)))
    hidden = inputs + low_back(product(context, output_weight)) + output_bias
    second = low(layer_norm(hidden, feed_gain, feed_shift))
    upward = low_back(product(second, upward_weight) + upward_bias)
    activated = low(jax.nn.gelu(upward, approximate=True))
    return hidden + low_back(product(activated, down_weight)) + down_bias

def reference(tokens, segment_ids, attention_gain, attention_shift, heads_weight, heads_bias, output_weight, output_bias, feed_gain, feed_shift, upward_weight, upward_bias, down_weight, down_bias, cotangent):
    param_set = tuple((element.astype(jnp.float32) for element in (attention_gain, attention_shift, heads_weight, heads_bias, output_weight, output_bias, feed_gain, feed_shift, upward_weight, upward_bias, down_weight, down_bias)))
    blocks = SEQS // GROUP_SEQS
    rows_block = GROUP_SEQS * SEQ_LEN
    inputs = tokens.astype(jnp.float32).reshape(blocks, rows_block, D)
    cotangents = cotangent.astype(jnp.float32).reshape(blocks, rows_block, D)
    segments = segment_ids.reshape(blocks, GROUP_SEQS, SEQ_LEN)

    def block_step(totals, element):
        block_input, block_cot, block_seg = element
        result, puller = jax.vjp(lambda first_in, params_in: forward(first_in, params_in, block_seg), block_input, param_set)
        input_part, param_grads = puller(block_cot)
        totals = jax.tree.map(lambda former, latter: former + latter, totals, param_grads)
        return (totals, (result, input_part))
    initial = jax.tree.map(jnp.zeros_like, param_set)
    totals, (results, input_parts) = lax.scan(block_step, initial, (inputs, cotangents, segments))
    layer_output = results.reshape(tokens.shape).astype(jnp.bfloat16)
    input_grad = input_parts.reshape(tokens.shape).astype(jnp.bfloat16)
    return (layer_output, input_grad, totals[0], totals[1], totals[2], totals[3], totals[4], totals[5], totals[6], totals[7], totals[8], totals[9], totals[10], totals[11])
```

```python
import jax
import jax.numpy as jnp
from jax import lax
from jax.sharding import PartitionSpec as P

HD = 128


EPSILON = 1e-05
NEGATIVE = -1e30


def normalize(values_in):
    center = values_in - jnp.mean(values_in, axis=-1, keepdims=True)
    spread = jnp.mean(center * center, axis=-1, keepdims=True)
    inverse = lax.rsqrt(spread + EPSILON)
    return (center * inverse, inverse)


def norm_back(upstream, normed, inverse, gain):
    scaled = upstream * gain
    return inverse * (
        scaled
        - jnp.mean(scaled, axis=-1, keepdims=True)
        - normed * jnp.mean(scaled * normed, axis=-1, keepdims=True)
    )


def matmul(former, latter):
    return jnp.dot(former, latter, preferred_element_type=jnp.float32)


def contract_rows(former, latter):
    return lax.dot_general(
        former, latter, (((0,), (0,)), ((), ())), preferred_element_type=jnp.float32
    )


def contract_cols(former, latter):
    return lax.dot_general(
        former, latter, (((1,), (1,)), ((), ())), preferred_element_type=jnp.float32
    )


def seq_mask(segments, places):
    return (segments[:, None] == segments[None, :]) & (places[None, :] <= places[:, None])


def masked_scores(queries, keys_all, segments, places):
    scaling = queries.shape[-1] ** (-0.5)
    scores = (
        jnp.einsum("qhd,khd->hqk", queries, keys_all, preferred_element_type=jnp.float32) * scaling
    )
    return (jnp.where(seq_mask(segments, places)[None], scores, NEGATIVE), scaling)


def attend_forward(inputs):
    queries, keys_all, values_all, segments, places = inputs
    scores, scaling = masked_scores(queries, keys_all, segments, places)
    highest = jnp.max(scores, axis=-1, keepdims=True)
    exponent = jnp.exp(scores - highest)
    totals = jnp.sum(exponent, axis=-1, keepdims=True)
    weights = (exponent / totals).astype(jnp.bfloat16)
    context = jnp.einsum(
        "hqk,khd->qhd", weights, values_all, preferred_element_type=jnp.float32
    ).astype(jnp.bfloat16)
    return (context, (highest + jnp.log(totals))[..., 0])


def attend_backward(inputs):
    queries, keys_all, values_all, segments, places, upstream, logsum = inputs
    scores, scaling = masked_scores(queries, keys_all, segments, places)
    weights = jnp.exp(scores - logsum[..., None])
    weights_grad = jnp.einsum(
        "qhd,khd->hqk", upstream, values_all, preferred_element_type=jnp.float32
    )
    weighted_sum = jnp.sum(weights_grad * weights, axis=-1, keepdims=True)
    scores_grad = (weights * (weights_grad - weighted_sum)).astype(jnp.bfloat16)
    query_grad = (
        jnp.einsum("hqk,khd->qhd", scores_grad, keys_all, preferred_element_type=jnp.float32)
        * scaling
    ).astype(jnp.bfloat16)
    key_grad = (
        jnp.einsum("hqk,qhd->khd", scores_grad, queries, preferred_element_type=jnp.float32)
        * scaling
    ).astype(jnp.bfloat16)
    value_grad = jnp.einsum(
        "hqk,qhd->khd", weights.astype(jnp.bfloat16), upstream, preferred_element_type=jnp.float32
    ).astype(jnp.bfloat16)
    return (query_grad, key_grad, value_grad)


ORDERS = ((0, 1, 2, 3), (1, 0, 2, 3), (2, 3, 1, 0), (3, 2, 1, 0))
PARTNERS = ((0, 1), (1, 0), (2, 3), (3, 2))
MIDDLE = ((1, 2), (2, 1))
OUTWARD = ((1, 0), (2, 3))
INWARD = ((0, 1), (3, 2))
ACROSS = ((1, 3), (2, 0))


def permute(values_in, pairs):
    return lax.ppermute(values_in, "tensor", pairs)


def gather_line(own):
    partner = permute(own, PARTNERS)
    near = permute(own, MIDDLE)
    far = permute(partner, MIDDLE)
    near = near + permute(near, OUTWARD)
    far = far + permute(far, OUTWARD)
    return [own, partner, near, far]


def scatter_line(blocks):
    own, partner, near, far = blocks
    low = jnp.bfloat16
    far_in = permute(far.astype(low), INWARD)
    near_in = permute(near.astype(low), INWARD)
    from_partner = permute(partner.astype(low), PARTNERS)
    far_sum = (far.astype(jnp.float32) + far_in.astype(jnp.float32)).astype(low)
    from_far = permute(far_sum, ACROSS)
    near_sum = (near.astype(jnp.float32) + near_in.astype(jnp.float32)).astype(low)
    from_near = permute(near_sum, MIDDLE)
    total = own.astype(jnp.float32) + from_partner.astype(jnp.float32)
    return total + from_far.astype(jnp.float32) + from_near.astype(jnp.float32)


def after(value, *others):
    return lax.optimization_barrier((value,) + others)[0]


def shards(
    tokens,
    segment_ids,
    attention_gain,
    attention_shift,
    heads_weight,
    heads_bias,
    output_weight,
    output_bias,
    feed_gain,
    feed_shift,
    upward_weight,
    upward_bias,
    down_weight,
    down_bias,
    cotangent,
):
    members = lax.axis_size("tensor")
    owners = lax.axis_size("fsdp")
    sequences, length = segment_ids.shape
    line = members == 4 and sequences == 1
    rows, width = tokens.shape
    low = jnp.bfloat16

    def gather(own):
        if line:
            return jnp.concatenate(gather_line(own), axis=0)
        return lax.all_gather(own, "tensor", axis=0, tiled=True)

    def scatter(partial):
        if line:
            return scatter_line([partial[i * rows : (i + 1) * rows] for i in range(4)])
        return lax.psum_scatter(
            partial.astype(low), "tensor", scatter_dimension=0, tiled=True
        ).astype(jnp.float32)

    if line:
        order = jnp.asarray(ORDERS, jnp.int32)[lax.axis_index("tensor")]
        places = (order[:, None] * rows + jnp.arange(rows, dtype=jnp.int32)[None]).reshape(1, length)
        segments = segment_ids.reshape(4, rows)[order].reshape(1, length)
    else:
        places = jnp.broadcast_to(jnp.arange(length, dtype=jnp.int32), segment_ids.shape)
        segments = segment_ids

    small = [
        attention_gain,
        attention_shift,
        output_bias,
        feed_gain,
        feed_shift,
        down_bias,
        upward_bias,
        heads_bias[0],
        heads_bias[1],
    ]
    packed = jnp.concatenate(small)
    packed = lax.all_gather(packed, "fsdp", axis=0, tiled=False)
    vectors_full = []
    at = 0
    for vector in small:
        size = vector.shape[0]
        vectors_full.append(packed[:, at : at + size].reshape(-1).astype(jnp.float32))
        at += size
    gain_one, shift_one, outbias, gain_two, shift_two, downbias, upbias, qbias, vbias = vectors_full

    heads_full = lax.all_gather(heads_weight, "fsdp", axis=1, tiled=True)
    output_full = lax.all_gather(output_weight, "fsdp", axis=1, tiled=True)
    upward_full = lax.all_gather(upward_weight, "fsdp", axis=0, tiled=True)
    down_full = lax.all_gather(down_weight, "fsdp", axis=1, tiled=True)

    inputs = tokens.astype(jnp.float32)
    normed_one, inverse_one = normalize(inputs)
    scaled_one = (normed_one * gain_one + shift_one).astype(low)
    gathered_one = gather(scaled_one)
    upstream = gather(after(cotangent, gathered_one))
    group_rows = gathered_one.shape[0]
    projected = jnp.einsum(
        "td,edw->etw", gathered_one, heads_full, preferred_element_type=jnp.float32
    )
    queries = (projected[0] + qbias).astype(low)
    keys_all = projected[1].astype(low)
    values_all = (projected[2] + vbias).astype(low)
    head_width = queries.shape[1]
    head_count = head_width // HD

    def split_heads(stacked_in):
        return stacked_in.reshape(sequences, length, head_count, HD)

    context, logsums = lax.map(
        attend_forward,
        (split_heads(queries), split_heads(keys_all), split_heads(values_all), segments, places),
    )
    context = context.reshape(group_rows, head_width)
    mixed_rows = scatter(matmul(context, output_full).astype(low))
    hidden = inputs + mixed_rows + outbias
    normed_two, inverse_two = normalize(hidden)
    scaled_two = (normed_two * gain_two + shift_two).astype(low)
    gathered_two = gather(scaled_two)
    upward = matmul(gathered_two, upward_full) + upbias
    activated = jax.nn.gelu(upward, approximate=True).astype(low)
    units_grad = contract_cols(upstream, down_full)
    _, puller = jax.vjp(lambda element: jax.nn.gelu(element, approximate=True), upward)
    upward_rows_grad = puller(units_grad)[0].astype(low)
    scaled_two_grad = scatter(contract_cols(upward_rows_grad, upward_full).astype(low))
    down_grad = contract_rows(activated, upstream).astype(low)
    upward_grad = contract_rows(gathered_two, upward_rows_grad).astype(low)
    upbias_grad = jnp.sum(upward_rows_grad, axis=0, dtype=jnp.float32)
    down_shard = lax.psum_scatter(down_grad, "fsdp", scatter_dimension=1, tiled=True)
    upward_shard = lax.psum_scatter(upward_grad, "fsdp", scatter_dimension=0, tiled=True)
    cot_local = cotangent.astype(jnp.float32)
    gain_two_grad = jnp.sum(scaled_two_grad * normed_two, axis=0)
    shift_two_grad = jnp.sum(scaled_two_grad, axis=0)
    downbias_grad = jnp.sum(cot_local, axis=0)
    hidden_grad = cot_local + norm_back(scaled_two_grad, normed_two, inverse_two, gain_two)
    outbias_grad = jnp.sum(hidden_grad, axis=0)
    upstream_two = gather(hidden_grad.astype(low))
    down_partial = after(matmul(activated, down_full).astype(low), upstream_two)
    result = hidden + scatter(down_partial) + downbias
    layer_output = result.astype(low)
    context_grad = contract_cols(upstream_two, output_full).astype(low)
    output_grad = contract_rows(context, upstream_two).astype(low)
    output_shard = lax.psum_scatter(output_grad, "fsdp", scatter_dimension=1, tiled=True)
    query_grad, key_grad, value_grad = lax.map(
        attend_backward,
        (
            split_heads(queries),
            split_heads(keys_all),
            split_heads(values_all),
            segments,
            places,
            split_heads(context_grad),
            logsums,
        ),
    )
    stacked = jnp.stack(
        [
            query_grad.reshape(group_rows, head_width),
            key_grad.reshape(group_rows, head_width),
            value_grad.reshape(group_rows, head_width),
        ]
    )
    scaled_one_grad = scatter(
        jnp.einsum("etw,edw->td", stacked, heads_full, preferred_element_type=jnp.float32).astype(low)
    )
    heads_grad = jnp.einsum(
        "td,etw->edw", gathered_one, stacked, preferred_element_type=jnp.float32
    ).astype(low)
    heads_shard = lax.psum_scatter(heads_grad, "fsdp", scatter_dimension=1, tiled=True)
    qbias_grad = jnp.sum(stacked[0], axis=0, dtype=jnp.float32)
    vbias_grad = jnp.sum(stacked[2], axis=0, dtype=jnp.float32)
    gain_one_grad = jnp.sum(scaled_one_grad * normed_one, axis=0)
    shift_one_grad = jnp.sum(scaled_one_grad, axis=0)
    input_grad = (
        hidden_grad + norm_back(scaled_one_grad, normed_one, inverse_one, gain_one)
    ).astype(low)
    vectors = jnp.stack(
        [gain_one_grad, shift_one_grad, outbias_grad, gain_two_grad, shift_two_grad, downbias_grad]
    )
    biases = jnp.concatenate(
        [vector.reshape(owners, -1) for vector in (upbias_grad, qbias_grad, vbias_grad)], axis=1
    )
    wide = vectors.reshape(6, owners, -1).transpose(1, 0, 2).reshape(owners, -1)
    wide = lax.psum(wide, "tensor")
    joined = jnp.concatenate([wide, biases], axis=1)
    joined = lax.psum_scatter(joined, "fsdp", scatter_dimension=0, tiled=True).reshape(-1)
    per = width // owners
    vector_total = joined[: 6 * per].reshape(6, per)
    at = 6 * per
    upbias_shard = joined[at : at + upward_bias.shape[0]]
    headbias_shard = joined[at + upward_bias.shape[0] :].reshape(2, -1)
    full = jnp.float32
    return (
        layer_output,
        input_grad,
        vector_total[0],
        vector_total[1],
        heads_shard.astype(full),
        headbias_shard,
        output_shard.astype(full),
        vector_total[2],
        vector_total[3],
        vector_total[4],
        upward_shard.astype(full),
        upbias_shard,
        down_shard.astype(full),
        vector_total[5],
    )


def solution(mesh):
    return jax.shard_map(
        shards,
        mesh=mesh,
        in_specs=(
            P(("fsdp", "tensor"), None),
            P("fsdp", None),
            P("fsdp"),
            P("fsdp"),
            P(None, "fsdp", "tensor"),
            P(None, ("tensor", "fsdp")),
            P("tensor", "fsdp"),
            P("fsdp"),
            P("fsdp"),
            P("fsdp"),
            P("fsdp", "tensor"),
            P(("tensor", "fsdp")),
            P("tensor", "fsdp"),
            P("fsdp"),
            P(("fsdp", "tensor"), None),
        ),
        out_specs=(
            P(("fsdp", "tensor"), None),
            P(("fsdp", "tensor"), None),
            P("fsdp"),
            P("fsdp"),
            P(None, "fsdp", "tensor"),
            P(None, ("tensor", "fsdp")),
            P("tensor", "fsdp"),
            P("fsdp"),
            P("fsdp"),
            P("fsdp"),
            P("fsdp", "tensor"),
            P(("tensor", "fsdp")),
            P("tensor", "fsdp"),
            P("fsdp"),
        ),
        check_vma=False,
    )
```
